8 devices in a mesh: dp: 1 (over z), pp: 8 (over y, x, core).
Axes of the slice: x: 2, y: 2, z: 1, core: 2. Of those that a mesh axis runs over, the one named last changes fastest.
Arguments:
- tokens: int32 [16, 2, 128], P('dp')
- targets: int32 [16, 2, 128], P('dp')
- emb: bfloat16 [49152, 2048], replicated
- g_final: bfloat16 [2048], replicated
- active: int32 [8, 1], P('pp')
- g_attn: bfloat16 [8, 1, 2048], P('pp')
- w_q: bfloat16 [8, 1, 2048, 2048], P('pp')
- w_k: bfloat16 [8, 1, 2048, 2048], P('pp')
- w_v: bfloat16 [8, 1, 2048, 2048], P('pp')
- w_o: bfloat16 [8, 1, 32, 64, 2048], P('pp')
- g_mlp: bfloat16 [8, 1, 2048], P('pp')
- w_gate: bfloat16 [8, 1, 2048, 8192], P('pp')
- w_up: bfloat16 [8, 1, 2048, 8192], P('pp')
- w_down: bfloat16 [8, 1, 8192, 2048], P('pp')
Outputs:
- output 1: float32 [16, 2, 128], P('dp')
- output 2: float32 [16], P('dp')
All inputs are finite; a program needn't handle non-finite values.
Results may differ from the reference program's by a relative error of at most 0.00352521.
Values are sent between devices in bfloat16 or wider.
A program may use at most 1.5 GiB of HBM per device.

```python
import math
import jax
import jax.numpy as jnp
from jax import lax

N_MICRO = 16
BATCH_SEQS = 2
SEQ_LEN = 128
STAGE_SLOTS = 1
N_STAGES = 8
D_MODEL = 2048
N_HEADS = 32
KV_HEADS = 32
HEAD_DIM = 64
FFN_DIM = 8192
VOCAB_SIZE = 49152

NORM_EPS = 1e-5
ROPE_BASE = 500000.0
ROPE_FACTOR = 32.0
ROPE_LOW = 1.0
ROPE_HIGH = 4.0
ROPE_ORIG = 8192.0


def setup_inputs(seed: int = 0, part: int = 0) -> dict:
    shared = jax.random.split(jax.random.key(seed), 12)
    data_keys = jax.random.split(jax.random.fold_in(jax.random.key(seed + 1), part), 2)
    stack = (N_STAGES, STAGE_SLOTS)
    q_width = N_HEADS * HEAD_DIM
    kv_width = KV_HEADS * HEAD_DIM
    d_scale = D_MODEL ** -0.5

    def normal(key, shape, scale):
        return (jax.random.normal(key, shape, jnp.float32) * scale).astype(jnp.bfloat16)

    def gains(key, shape, scale):
        return ((1.0 + 0.3 * jax.random.normal(key, shape, jnp.float32)) * scale).astype(jnp.bfloat16)

    slot_ids = jnp.arange(N_STAGES * STAGE_SLOTS, dtype=jnp.int32).reshape(stack)
    ends = (slot_ids == 0) | (slot_ids == N_STAGES * STAGE_SLOTS - 1)
    coins = jax.random.randint(shared[2], stack, 0, 4, dtype=jnp.int32)
    active = jnp.where(ends | (coins == 0), 0, 1).astype(jnp.int32)
    id_shape = (N_MICRO, BATCH_SEQS, SEQ_LEN)
    return {
        "tokens": jax.random.randint(data_keys[0], id_shape, 0, VOCAB_SIZE, dtype=jnp.int32),
        "targets": jax.random.randint(data_keys[1], id_shape, 0, VOCAB_SIZE, dtype=jnp.int32),
        "emb": normal(shared[0], (VOCAB_SIZE, D_MODEL), 1.0),
        "g_final": gains(shared[1], (D_MODEL,), 3.0 / math.sqrt(D_MODEL)),
        "active": active,
        "g_attn": gains(shared[3], stack + (D_MODEL,), 1.0),
        "w_q": normal(shared[4], stack + (D_MODEL, q_width), 1.6 * d_scale),
        "w_k": normal(shared[5], stack + (D_MODEL, kv_width), 1.6 * d_scale),
        "w_v": normal(shared[6], stack + (D_MODEL, kv_width), d_scale),
        "w_o": normal(shared[7], stack + (N_HEADS, HEAD_DIM, D_MODEL), q_width ** -0.5),
        "g_mlp": gains(shared[8], stack + (D_MODEL,), 1.0),
        "w_gate": normal(shared[9], stack + (D_MODEL, FFN_DIM), d_scale),
        "w_up": normal(shared[10], stack + (D_MODEL, FFN_DIM), d_scale),
        "w_down": normal(shared[11], stack + (FFN_DIM, D_MODEL), FFN_DIM ** -0.5),
    }


def rope_tables():
    half_dim = HEAD_DIM // 2
    inv_freq = ROPE_BASE ** (-2.0 * jnp.arange(half_dim, dtype=jnp.float32) / HEAD_DIM)
    wavelen = 2.0 * math.pi / inv_freq
    smooth = jnp.clip((ROPE_ORIG / wavelen - ROPE_LOW) / (ROPE_HIGH - ROPE_LOW), 0.0, 1.0)
    scaled_freq = (1.0 - smooth) * inv_freq / ROPE_FACTOR + smooth * inv_freq
    angles = jnp.arange(SEQ_LEN, dtype=jnp.float32)[:, None] * scaled_freq[None, :]
    return jnp.cos(angles), jnp.sin(angles)


def rotate(proj, cos_t, sin_t):
    half_dim = proj.shape[-1] // 2
    table_shape = (cos_t.shape[0],) + (1,) * (proj.ndim - 3) + (half_dim,)
    cos_b = cos_t.reshape(table_shape)
    sin_b = sin_t.reshape(table_shape)
    first = proj[..., :half_dim]
    second = proj[..., half_dim:]
    return jnp.concatenate([first * cos_b - second * sin_b, second * cos_b + first * sin_b], axis=-1)


def rms_norm(hidden, gain):
    hidden_wide = hidden.astype(jnp.float32)
    inv_rms = lax.rsqrt(jnp.mean(hidden_wide * hidden_wide, axis=-1, keepdims=True) + NORM_EPS)
    return (hidden_wide * inv_rms * gain.astype(jnp.float32)).astype(jnp.bfloat16)


def decoder_layer(hidden, weights, cos_t, sin_t):
    g_attn, w_q, w_k, w_v, w_o, g_mlp, w_gate, w_up, w_down = weights
    tok_count = BATCH_SEQS * SEQ_LEN
    groups = N_HEADS // KV_HEADS
    normed = rms_norm(hidden, g_attn).reshape(tok_count, D_MODEL)
    query = jnp.dot(normed, w_q, preferred_element_type=jnp.float32).reshape(BATCH_SEQS, SEQ_LEN, N_HEADS, HEAD_DIM)
    keys = jnp.dot(normed, w_k, preferred_element_type=jnp.float32).reshape(BATCH_SEQS, SEQ_LEN, KV_HEADS, HEAD_DIM)
    values = jnp.dot(normed, w_v, preferred_element_type=jnp.float32).astype(jnp.bfloat16).reshape(BATCH_SEQS, SEQ_LEN, KV_HEADS, HEAD_DIM)
    query = rotate(query, cos_t, sin_t).astype(jnp.bfloat16).reshape(BATCH_SEQS, SEQ_LEN, KV_HEADS, groups, HEAD_DIM)
    keys = rotate(keys, cos_t, sin_t).astype(jnp.bfloat16)
    scores = jnp.einsum("bqngk,bsnk->bngqs", query.astype(jnp.float32), keys.astype(jnp.float32)) * (HEAD_DIM ** -0.5)
    positions = jnp.arange(SEQ_LEN)
    causal = positions[:, None] >= positions[None, :]
    scores = jnp.where(causal, scores, -1e30)
    attn_probs = jax.nn.softmax(scores, axis=-1).astype(jnp.bfloat16)
    context = jnp.einsum("bngqs,bsnk->bqngk", attn_probs.astype(jnp.float32), values.astype(jnp.float32)).astype(jnp.bfloat16)
    attn_out = jnp.dot(context.reshape(tok_count, N_HEADS * HEAD_DIM), w_o.reshape(N_HEADS * HEAD_DIM, D_MODEL), preferred_element_type=jnp.float32)
    hidden = (hidden.astype(jnp.float32) + attn_out.reshape(BATCH_SEQS, SEQ_LEN, D_MODEL)).astype(jnp.bfloat16)
    normed = rms_norm(hidden, g_mlp).reshape(tok_count, D_MODEL)
    gate_proj = jnp.dot(normed, w_gate, preferred_element_type=jnp.float32)
    up_proj = jnp.dot(normed, w_up, preferred_element_type=jnp.float32)
    hidden_act = (jax.nn.silu(gate_proj) * up_proj).astype(jnp.bfloat16)
    down_proj = jnp.dot(hidden_act, w_down, preferred_element_type=jnp.float32)
    return (hidden.astype(jnp.float32) + down_proj.reshape(BATCH_SEQS, SEQ_LEN, D_MODEL)).astype(jnp.bfloat16)


def head_loss(hidden, g_final, emb, targets):
    rows = math.gcd(SEQ_LEN, max(256 // BATCH_SEQS, 1))
    normed = rms_norm(hidden, g_final)

    def block_loss(index):
        start = index * rows
        z_block = lax.dynamic_slice_in_dim(normed, start, rows, axis=1).reshape(BATCH_SEQS * rows, D_MODEL)
        t_block = lax.dynamic_slice_in_dim(targets, start, rows, axis=1).reshape(BATCH_SEQS * rows)
        logits = lax.dot_general(z_block, emb, (((1,), (1,)), ((), ())), preferred_element_type=jnp.float32)
        picked = jnp.sum(z_block.astype(jnp.float32) * jnp.take(emb, t_block, axis=0).astype(jnp.float32), axis=-1)
        return (jax.nn.logsumexp(logits, axis=-1) - picked).reshape(BATCH_SEQS, rows)

    per_block = lax.map(block_loss, jnp.arange(SEQ_LEN // rows))
    return jnp.moveaxis(per_block, 0, 1).reshape(BATCH_SEQS, SEQ_LEN)


def reference(tokens, targets, emb, g_final, active, g_attn, w_q, w_k, w_v, w_o, g_mlp, w_gate, w_up, w_down):
    slot_count = N_STAGES * STAGE_SLOTS
    stacked = tuple(w.reshape((slot_count,) + w.shape[2:]) for w in (g_attn, w_q, w_k, w_v, w_o, g_mlp, w_gate, w_up, w_down))
    flags = active.reshape(slot_count)
    cos_t, sin_t = rope_tables()

    def keep(hidden):
        return hidden

    def slot_step(hidden, slot_in):
        flag, weights = slot_in
        hidden = lax.cond(flag != 0, lambda h: decoder_layer(h, weights, cos_t, sin_t), keep, hidden)
        return hidden, None

    def one_micro(pair):
        tok_ids, tgt_ids = pair
        hidden = jnp.take(emb, tok_ids, axis=0)
        hidden, _ = lax.scan(slot_step, hidden, (flags, stacked))
        return head_loss(hidden, g_final, emb, tgt_ids)

    token_loss = lax.map(one_micro, (tokens, targets))
    return token_loss, jnp.mean(token_loss, axis=(1, 2))
```

```python
import functools
import math

import jax
import jax.numpy as jnp
from jax import lax
from jax.experimental import pallas as pl
from jax.experimental.pallas import tpu as pltpu
from jax.sharding import PartitionSpec as P

BF = jnp.bfloat16
F32 = jnp.float32
NORM_EPS = 1e-5
ROPE_BASE = 500000.0
ROPE_FACTOR = 32.0
ROPE_LOW = 1.0
ROPE_HIGH = 4.0
ROPE_ORIG = 8192.0

NMB = 16
ROWS = 256
D = 2048
FFN = 8192
VOCAB = 49152
CH = 512
NC = D // CH
NG = 3
BODIES = 17
FIRST, LAST = 1, 6
HG = 2048
HEAD_GROUPS = VOCAB // 2 // HG
FIN_GROUPS = VOCAB // 6 // HG
MESH = pl.DeviceIdType.MESH


def rope_tables():
    half = 32
    inv_freq = ROPE_BASE ** (-2.0 * jnp.arange(half, dtype=F32) / (2 * half))
    wavelen = 2.0 * math.pi / inv_freq
    smooth = jnp.clip((ROPE_ORIG / wavelen - ROPE_LOW) / (ROPE_HIGH - ROPE_LOW), 0.0, 1.0)
    scaled = (1.0 - smooth) * inv_freq / ROPE_FACTOR + smooth * inv_freq
    angles = jnp.arange(128, dtype=F32)[:, None] * scaled[None, :]
    c, s = jnp.cos(angles), jnp.sin(angles)
    z = jnp.zeros_like(s)
    cos = jnp.tile(c, (1, 4))
    sin_a = jnp.tile(jnp.concatenate([-s, z], 1), (1, 2))
    sin_b = jnp.tile(jnp.concatenate([z, s], 1), (1, 2))
    t = jnp.stack([cos, sin_a, sin_b])
    return jnp.concatenate([t * 0.125, t], 0)


def dotf(a, b):
    return jnp.dot(a, b, preferred_element_type=F32)


def dott(a, b):
    return lax.dot_general(a, b, (((1,), (1,)), ((), ())), preferred_element_type=F32)


def norm_rows(src, g_ref, dst):
    gains = [g_ref[:, CH * c:CH * (c + 1)].astype(F32) for c in range(NC)]

    def block(i, _):
        r0 = pl.multiple_of(i * 64, 64)
        for u in range(4):
            rows = pl.ds(r0 + 16 * u, 16)
            ss = None
            for c in range(NC):
                xv = src[c, rows, :].astype(F32)
                sq = xv * xv
                part = sq[:, :128] + sq[:, 128:256] + sq[:, 256:384] + sq[:, 384:]
                ss = part if ss is None else ss + part
            inv = lax.rsqrt(jnp.sum(ss, axis=1, keepdims=True) * (1.0 / D) + NORM_EPS)
            for c in range(NC):
                xv = src[c, rows, :].astype(F32)
                dst[rows, CH * c:CH * (c + 1)] = (xv * inv * gains[c]).astype(BF)
        return 0

    lax.fori_loop(0, ROWS // 64, block, 0)


def rope(y, tab, base):
    rows = []
    for s in range(2):
        cols = []
        for j in range(CH // 128):
            v = y[128 * s:128 * (s + 1), 128 * j:128 * (j + 1)]
            cols.append(v * tab[base] + pltpu.roll(v, 96, 1) * tab[base + 1] + pltpu.roll(v, 32, 1) * tab[base + 2])
        rows.append(jnp.concatenate(cols, axis=1))
    return jnp.concatenate(rows, axis=0)


def attend_probs(q, k, ch, pair, seq, lo, causal):
    rows, cols = pl.ds(128 * seq, 128), pl.ds(128 * pair, 128)
    qp, kp = q[ch, rows, cols], k[ch, rows, cols]
    zero = jnp.zeros((128, 128), BF)
    both = jnp.concatenate([jnp.where(lo, kp, zero), jnp.where(lo, zero, kp)], axis=0)
    scores = dott(qp, both)
    probs = []
    for head in range(2):
        z = jnp.where(causal, scores[:, 128 * head:128 * (head + 1)], -1e30)
        e = jnp.exp(z - jnp.max(z, axis=1, keepdims=True))
        probs.append((e * (1.0 / jnp.sum(e, axis=1, keepdims=True))).astype(BF))
    return jnp.concatenate(probs, axis=1)


def attend_values(q, v, ch, pair, seq, lo, probs):
    rows, cols = pl.ds(128 * seq, 128), pl.ds(128 * pair, 128)
    vp = v[ch, rows, cols]
    zero = jnp.zeros((128, 128), BF)
    both = jnp.concatenate([jnp.where(lo, vp, zero), jnp.where(lo, zero, vp)], axis=0)
    q[ch, rows, cols] = dotf(probs, both).astype(BF)


def kernel(x_hbm, emb, gf, tgt, ga, gm, wq, wk, wv, wo, wg, wu, wd, tab, flag, out,
           ring, res, xin, xfin, x1, h, q, k, v, a, xout, st, stf,
           wsem, rsem, xsem, recv_sem, send_sem, send0_sem, free_sem, free0_sem,
           fsend_sem, frecv_sem, ffwd_sem, ssend_sem, srecv_sem, tsend_sem, trecv_sem):
    me = lax.axis_index("pp")
    is_layer = jnp.logical_and(me >= FIRST, me <= LAST)
    is_head = jnp.logical_or(me == 0, me == 7)
    lane = lax.broadcasted_iota(jnp.int32, (128, 128), 1)
    lo = lane < 64
    causal = lax.broadcasted_iota(jnp.int32, (128, 128), 0) >= lane
    units = [(p, s) for p in range(4) for s in range(2)]

    def al(i, n):
        return i if isinstance(i, int) else pl.multiple_of(i, n)

    def slot_of(m, b):
        return lax.rem(BODIES * m + b, NG)

    def load(src, slot, t):
        pltpu.make_async_copy(src, ring.at[slot, t], wsem.at[slot]).start()

    def load_res(src, i):
        pltpu.make_async_copy(src, res.at[i], rsem.at[i]).start()

    def wait_group(slot):
        pltpu.make_async_copy(ring.at[slot], ring.at[slot], wsem.at[slot]).wait()

    def wait_res(i):
        pltpu.make_async_copy(res.at[i], res.at[i], rsem.at[i]).wait()

    def cols_of(w, c):
        return w.at[:, pl.ds(al(c * CH, CH), CH)]

    def start_qkv(i, slot):
        for t, w in enumerate((wq, wk, wv)):
            load(cols_of(w, i), slot, t)

    def start_out(slot):
        for t in range(3):
            load(cols_of(wo, t), slot, t)

    def start_ffn(c, slot):
        load(cols_of(wg, 2 * c), slot, 0)
        load(cols_of(wg, 2 * c + 1), slot, 1)
        load(cols_of(wu, 2 * c), slot, 2)

    def down_tile(n, t):
        return wd.at[pl.ds(D * t, D), pl.ds(al(n * CH, CH), CH)]

    def start_down(n, slot):
        for t in range(3):
            load(down_tile(n, t), slot, t)

    def to_next(s, n):
        return pltpu.make_async_remote_copy(xout.at[s, n], xin.at[s, n], send_sem.at[s, n], recv_sem.at[s, n],
                                            device_id={"pp": lax.rem(me + 1, 8)}, device_id_type=MESH)

    def to_zero(s, n):
        return pltpu.make_async_remote_copy(xout.at[s, n], xin.at[s, n], send0_sem.at[s, n], recv_sem.at[s, n],
                                            device_id={"pp": 0}, device_id_type=MESH)

    fin_targets = (7, 4, 2)

    def to_fin(i, s, n):
        return pltpu.make_async_remote_copy(xout.at[s, n], xfin.at[n], fsend_sem.at[i, n], frecv_sem.at[n],
                                            device_id={"pp": fin_targets[i]}, device_id_type=MESH)

    def forward(n):
        return pltpu.make_async_remote_copy(xfin.at[n], xfin.at[n], ffwd_sem.at[n], frecv_sem.at[n],
                                            device_id={"pp": lax.rem(me + 1, 8)}, device_id_type=MESH)

    def load_x(m, s, c):
        return pltpu.make_async_copy(x_hbm.at[m, :, pl.ds(CH * c, CH)], xin.at[s, c], xsem.at[s, c])

    def start_head(row, slot):
        for t in range(4):
            pltpu.make_async_copy(emb.at[pl.ds(al(row, HG), HG), pl.ds(CH * t, CH)], res.at[4 * slot + t], rsem.at[slot]).start()

    def wait_head(slot):
        view = res.at[pl.ds(4 * slot, 4)]
        pltpu.make_async_copy(view, view, rsem.at[slot]).wait()

    sub8 = lax.broadcasted_iota(jnp.int32, (8, ROWS), 0)

    def head_group(slot, row, y, carry):
        mx, sm, pk = carry
        yrel = y - row - sub8
        for nb in range(HG // CH):
            lg = None
            for t in range(4):
                part = dott(res[4 * slot + t, CH * nb:CH * (nb + 1), :], h[:, CH * t:CH * (t + 1)])
                lg = part if lg is None else lg + part
            l3 = lg.reshape(CH // 8, 8, ROWS)
            new = jnp.maximum(mx, jnp.max(l3, axis=0))
            sm = sm * jnp.exp(mx - new) + jnp.sum(jnp.exp(l3 - new[None]), axis=0)
            for r in range(CH // 8):
                pk = pk + jnp.where(yrel == CH * nb + 8 * r, l3[r], 0.0)
            mx = new
        return mx, sm, pk

    def head_start():
        return (jnp.full((8, ROWS), -3e38, F32), jnp.zeros((8, ROWS), F32), jnp.zeros((8, ROWS), F32))

    def head_stats(carry):
        mx, sm, pk = carry
        top = jnp.max(mx, axis=0, keepdims=True)
        tot = jnp.sum(sm * jnp.exp(mx - top), axis=0, keepdims=True)
        return top, tot, jnp.sum(pk, axis=0, keepdims=True)

    @pl.when(is_layer)
    def _():
        for i in range(3):
            start_qkv(i, i)

        @pl.when(me == FIRST)
        def _():
            for c in range(NC):
                load_x(0, 0, c).start()

        def one(m, _):
            s = lax.rem(m, 2)
            first = m == 0
            more = m < NMB - 1

            @pl.when(me == FIRST)
            def _():
                for c in range(NC):
                    load_x(m, s, c).wait()

                @pl.when(more)
                def _():
                    for c in range(NC):
                        load_x(m + 1, 1 - s, c).start()

            @pl.when(me != FIRST)
            def _():
                for c in range(NC):
                    to_next(s, c).wait_recv()

            norm_rows(xin.at[s], ga, h)
            on = flag[0:1, 0:1] != 0

            def qkv(i, prev):
                slot = slot_of(m, i)
                wait_group(slot)
                plan = [units[:4], units[4:], []] if prev is not None else [[], [], []]
                for j, dst in enumerate((q, k, v)):
                    ps = [attend_probs(q, k, prev, p, sq, lo, causal) for p, sq in plan[j]]
                    r = dotf(h[...], ring[slot, j])
                    if j < 2:
                        r = rope(r, tab, 3 * j)
                    dst[i] = r.astype(BF)
                    for (p, sq), pr in zip(plan[j], ps):
                        attend_values(q, v, prev, p, sq, lo, pr)
                return slot

            slot = qkv(0, None)
            start_qkv(3, slot)

            def qkv_loop(i, _):
                slot = qkv(i, i - 1)

                @pl.when(i == 1)
                def _():
                    start_out(slot)

                    @pl.when(first)
                    def _():
                        load_res(cols_of(wo, 3), 0)

                @pl.when(i > 1)
                def _():
                    start_ffn(i - 2, slot)

                    @pl.when(first)
                    def _():
                        load_res(cols_of(wu, 2 * (i - 2) + 1), 1 + i - 2)
                return 0

            lax.fori_loop(1, 4, qkv_loop, 0)
            ps = [attend_probs(q, k, 3, p, sq, lo, causal) for p, sq in units]
            for (p, sq), pr in zip(units, ps):
                attend_values(q, v, 3, p, sq, lo, pr)

            slot = slot_of(m, 4)
            wait_group(slot)

            @pl.when(first)
            def _():
                wait_res(0)

            for t in range(4):
                w = ring.at[slot, t] if t < 3 else res.at[0]
                r = None
                for kc in range(NC):
                    part = dotf(q[kc], w[CH * kc:CH * (kc + 1), :])
                    r = part if r is None else r + part
                xo = xin[s, t]
                x1[t] = jnp.where(on, (xo.astype(F32) + r).astype(BF), xo)
            start_ffn(2, slot)

            @pl.when(first)
            def _():
                load_res(cols_of(wu, 2 * 2 + 1), 1 + 2)

            @pl.when(jnp.logical_and(me != FIRST, m < NMB - 2))
            def _():
                pl.semaphore_signal(free_sem, 1, device_id={"pp": lax.rem(me + 7, 8)}, device_id_type=MESH)

            norm_rows(x1, gm, h)

            def ffn(c, _):
                slot = slot_of(m, 5 + c)
                wait_group(slot)

                @pl.when(first)
                def _():
                    wait_res(1 + c)

                for t in range(2):
                    gate = dotf(h[...], ring[slot, t])
                    up = dotf(h[...], ring[slot, 2] if t == 0 else res[1 + c])
                    a[c, :, CH * t:CH * (t + 1)] = (gate * (1.0 / (1.0 + jnp.exp(-gate))) * up).astype(BF)

                @pl.when(c < 5)
                def _():
                    start_ffn(c + 3, slot)

                    @pl.when(first)
                    def _():
                        load_res(cols_of(wu, 2 * (c + 3) + 1), 1 + c + 3)

                @pl.when(c >= 5)
                def _():
                    start_down(c - 5, slot)

                    @pl.when(first)
                    def _():
                        load_res(down_tile(c - 5, 3), 9 + c - 5)
                return 0

            lax.fori_loop(0, 8, ffn, 0)

            @pl.when(jnp.logical_and(m >= 2, jnp.logical_or(more, me != LAST)))
            def _():
                pl.semaphore_wait(free_sem, 1)

                @pl.when(me == LAST)
                def _():
                    pl.semaphore_wait(free0_sem, 1)

            def down(n, _):
                slot = slot_of(m, 13 + n)
                wait_group(slot)

                @pl.when(first)
                def _():
                    wait_res(9 + n)

                @pl.when(m >= 2)
                def _():
                    to_next(s, n).wait_send()

                    @pl.when(me == LAST)
                    def _():
                        to_zero(s, n).wait_send()

                acc = None
                for t in range(4):
                    w = ring.at[slot, t] if t < 3 else res.at[9 + n]
                    for u in range(2):
                        part = dotf(a[2 * t + u], w[1024 * u:1024 * (u + 1), :])
                        acc = part if acc is None else acc + part
                xo = x1[n]
                xout[s, n] = jnp.where(on, (xo.astype(F32) + acc).astype(BF), xo)

                @pl.when(jnp.logical_or(more, me != LAST))
                def _():
                    to_next(s, n).start()

                @pl.when(me == LAST)
                def _():
                    @pl.when(more)
                    def _():
                        to_zero(s, n).start()

                    @pl.when(jnp.logical_not(more))
                    def _():
                        for i in range(3):
                            to_fin(i, s, n).start()

                @pl.when(n == 0)
                def _():
                    start_down(3, slot)

                    @pl.when(first)
                    def _():
                        load_res(down_tile(3, 3), 12)

                @pl.when(jnp.logical_and(n > 0, more))
                def _():
                    start_qkv(n - 1, slot)
                return 0

            lax.fori_loop(0, NC, down, 0)
            return 0

        lax.fori_loop(0, NMB, one, 0)

    side = jnp.where(me == 7, 1, 0)
    base = side * (VOCAB // 2)

    def stats_to(i):
        return pltpu.make_async_remote_copy(st.at[side], st.at[side], ssend_sem.at[i], srecv_sem.at[side],
                                            device_id={"pp": lax.rem(me + 1 + i, 8)}, device_id_type=MESH)

    @pl.when(is_head)
    def _():
        for g in range(3):
            start_head(base + HG * g, g)

        def one(m, _):
            s = lax.rem(m, 2)
            for c in range(NC):
                to_next(s, c).wait_recv()
            norm_rows(xin.at[s], gf, h)

            @pl.when(m < NMB - 3)
            def _():
                @pl.when(me == 7)
                def _():
                    pl.semaphore_signal(free_sem, 1, device_id={"pp": LAST}, device_id_type=MESH)

                @pl.when(me == 0)
                def _():
                    pl.semaphore_signal(free0_sem, 1, device_id={"pp": LAST}, device_id_type=MESH)

            y = tgt[pl.ds(m, 1), :]

            def group(g, carry):
                slot = lax.rem(g, 3)
                wait_head(slot)
                row = base + HG * g
                carry = head_group(slot, row, y, carry)

                @pl.when(g < HEAD_GROUPS - 3)
                def _():
                    start_head(row + 3 * HG, slot)

                @pl.when(jnp.logical_and(g >= HEAD_GROUPS - 3, m < NMB - 2))
                def _():
                    start_head(row + 3 * HG - HG * HEAD_GROUPS, slot)
                return carry

            top, tot, pick = head_stats(lax.fori_loop(0, HEAD_GROUPS, group, head_start()))
            st[side, 0, pl.ds(m, 1), :] = top
            st[side, 1, pl.ds(m, 1), :] = tot
            st[side, 2, pl.ds(m, 1), :] = pick
            return 0

        lax.fori_loop(0, NMB - 1, one, 0)
        for j in range(3):
            st[side, j, NMB - 1:NMB, :] = jnp.ones((1, ROWS), F32)
        for i in range(7):
            stats_to(i).start()

    part = me - 2

    def fin_to(i):
        return pltpu.make_async_remote_copy(stf.at[part], stf.at[part], tsend_sem.at[i], trecv_sem.at[part],
                                            device_id={"pp": lax.rem(me + 1 + i, 8)}, device_id_type=MESH)

    @pl.when(me >= 2)
    def _():
        row0 = part * (HG * FIN_GROUPS)
        for g in range(3):
            start_head(row0 + HG * g, g)

        @pl.when(me == LAST)
        def _():
            for n in range(NC):
                xfin[n] = xout[(NMB - 1) % 2, n]

        @pl.when(me != LAST)
        def _():
            for n in range(NC):
                forward(n).wait_recv()

                @pl.when(jnp.logical_or(me == 2, me == 4))
                def _():
                    forward(n).start()

        norm_rows(xfin, gf, h)
        y = tgt[NMB - 1:NMB, :]

        def group(g, carry):
            slot = lax.rem(g, 3)
            wait_head(slot)
            row = row0 + HG * g
            carry = head_group(slot, row, y, carry)

            @pl.when(g < FIN_GROUPS - 3)
            def _():
                start_head(row + 3 * HG, slot)
            return carry

        top, tot, pick = head_stats(lax.fori_loop(0, FIN_GROUPS, group, head_start()))
        stf[part] = jnp.concatenate([top, tot, pick, jnp.zeros((5, ROWS), F32)], axis=0)
        for i in range(7):
            fin_to(i).start()

    for d in range(2):
        @pl.when(me != 7 * d)
        def _():
            pltpu.make_async_copy(st.at[d], st.at[d], srecv_sem.at[d]).wait()
    for f in range(6):
        @pl.when(me != f + 2)
        def _():
            pltpu.make_async_copy(stf.at[f], stf.at[f], trecv_sem.at[f]).wait()

    top = jnp.maximum(st[0, 0], st[1, 0])
    tot = st[0, 1] * jnp.exp(st[0, 0] - top) + st[1, 1] * jnp.exp(st[1, 0] - top)
    out[...] = jnp.log(tot) + top - (st[0, 2] + st[1, 2])
    ftop = stf[0, 0:1, :]
    for f in range(1, 6):
        ftop = jnp.maximum(ftop, stf[f, 0:1, :])
    ftot = jnp.zeros((1, ROWS), F32)
    fpick = jnp.zeros((1, ROWS), F32)
    for f in range(6):
        ftot = ftot + stf[f, 1:2, :] * jnp.exp(stf[f, 0:1, :] - ftop)
        fpick = fpick + stf[f, 2:3, :]
    out[NMB - 1:NMB, :] = jnp.log(ftot) + ftop - fpick

    @pl.when(is_layer)
    def _():
        for n in range(NC):
            to_next(0, n).wait_send()

            @pl.when(me != LAST)
            def _():
                to_next(1, n).wait_send()

            @pl.when(me == LAST)
            def _():
                to_zero(0, n).wait_send()
                for i in range(3):
                    to_fin(i, 1, n).wait_send()

    @pl.when(is_head)
    def _():
        for i in range(7):
            stats_to(i).wait_send()

    @pl.when(me >= 2)
    def _():
        for i in range(7):
            fin_to(i).wait_send()

        @pl.when(jnp.logical_or(me == 2, me == 4))
        def _():
            for n in range(NC):
                forward(n).wait_send()


def solution(mesh):
    def stage_program(tokens, targets, emb, g_final, active, g_attn, w_q, w_k, w_v, w_o, g_mlp, w_gate, w_up, w_down):
        x = jnp.take(emb, tokens.reshape(NMB * ROWS), axis=0).reshape(NMB, ROWS, D)
        flag = jnp.broadcast_to(active.reshape(1, 1), (8, 128))
        hbm = pl.BlockSpec(memory_space=pltpu.HBM)
        vmem = pl.BlockSpec(memory_space=pltpu.VMEM)
        dma, regular = pltpu.SemaphoreType.DMA, pltpu.SemaphoreType.REGULAR
        token_loss = pl.pallas_call(
            kernel,
            out_shape=jax.ShapeDtypeStruct((NMB, ROWS), F32),
            in_specs=[hbm, hbm, vmem, vmem, vmem, vmem] + [hbm] * 7 + [vmem, vmem],
            out_specs=vmem,
            scratch_shapes=[
                pltpu.VMEM((NG, 3, D, CH), BF),
                pltpu.VMEM((13, D, CH), BF),
                pltpu.VMEM((2, NC, ROWS, CH), BF),
                pltpu.VMEM((NC, ROWS, CH), BF),
                pltpu.VMEM((NC, ROWS, CH), BF),
                pltpu.VMEM((ROWS, D), BF),
                pltpu.VMEM((NC, ROWS, CH), BF),
                pltpu.VMEM((NC, ROWS, CH), BF),
                pltpu.VMEM((NC, ROWS, CH), BF),
                pltpu.VMEM((8, ROWS, 1024), BF),
                pltpu.VMEM((2, NC, ROWS, CH), BF),
                pltpu.VMEM((2, 3, NMB, ROWS), F32),
                pltpu.VMEM((6, 8, ROWS), F32),
                dma((NG,)), dma((13,)), dma((2, NC)), dma((2, NC)), dma((2, NC)), dma((2, NC)), regular, regular,
                dma((3, NC)), dma((NC,)), dma((NC,)), dma((7,)), dma((2,)), dma((7,)), dma((6,)),
            ],
            compiler_params=pltpu.CompilerParams(vmem_limit_bytes=67043328, has_side_effects=True),
        )(x, emb, g_final.reshape(1, D), targets.reshape(NMB, ROWS), g_attn.reshape(1, D), g_mlp.reshape(1, D),
          w_q.reshape(D, D), w_k.reshape(D, D), w_v.reshape(D, D), w_o.reshape(D, D),
          w_gate.reshape(D, FFN), w_up.reshape(D, FFN), w_down.reshape(FFN, D), rope_tables(), flag)
        return token_loss.reshape(NMB, 2, 128), jnp.mean(token_loss, axis=1)

    stack = P("pp")
    in_specs = (P("dp"), P("dp"), P(), P()) + (stack,) * 10
    return jax.shard_map(stage_program, mesh=mesh, in_specs=in_specs, out_specs=(P("dp"), P("dp")), check_vma=False)
```

```python
import functools
import math

import jax
import jax.numpy as jnp
import numpy as np
from jax import lax
from jax.experimental import pallas as pl
from jax.experimental.pallas import tpu as pltpu
from jax.sharding import PartitionSpec as P

BF = jnp.bfloat16
F32 = jnp.float32
NORM_EPS = 1e-5
ROPE_BASE = 500000.0
ROPE_FACTOR = 32.0
ROPE_LOW = 1.0
ROPE_HIGH = 4.0
ROPE_ORIG = 8192.0

NMB = 16
ROWS = 256
D = 2048
FFN = 8192
VOCAB = 49152
CH = 512
NC = D // CH
NG = 3
BODIES = 17
FIRST, LAST = 1, 6
HG = 2048
HEAD_GROUPS = VOCAB // 2 // HG
FIN_GROUPS = VOCAB // 6 // HG
MESH = pl.DeviceIdType.MESH


def rope_tables():
    half = 32
    inv_freq = ROPE_BASE ** (-2.0 * np.arange(half) / (2 * half))
    wavelen = 2.0 * math.pi / inv_freq
    smooth = np.clip((ROPE_ORIG / wavelen - ROPE_LOW) / (ROPE_HIGH - ROPE_LOW), 0.0, 1.0)
    scaled = (1.0 - smooth) * inv_freq / ROPE_FACTOR + smooth * inv_freq
    angles = np.arange(128)[:, None] * scaled[None, :]
    c, s = np.cos(angles), np.sin(angles)
    z = np.zeros_like(s)
    t = np.stack([np.tile(c, (1, 4)), np.tile(np.concatenate([-s, z], 1), (1, 2)), np.tile(np.concatenate([z, s], 1), (1, 2))])
    return np.concatenate([t * 0.125, t], 0).astype(np.float32)


def dotf(a, b):
    return jnp.dot(a, b, preferred_element_type=F32)


def dott(a, b):
    return lax.dot_general(a, b, (((1,), (1,)), ((), ())), preferred_element_type=F32)


def norm_rows(src, g_ref, dst):
    gains = [g_ref[:, CH * c:CH * (c + 1)].astype(F32) for c in range(NC)]

    def block(i, _):
        r0 = pl.multiple_of(i * 128, 128)
        for u in range(8):
            rows = pl.ds(r0 + 16 * u, 16)
            ss = None
            for c in range(NC):
                xv = src[c, rows, :].astype(F32)
                sq = xv * xv
                part = sq[:, :128] + sq[:, 128:256] + sq[:, 256:384] + sq[:, 384:]
                ss = part if ss is None else ss + part
            inv = lax.rsqrt(jnp.sum(ss, axis=1, keepdims=True) * (1.0 / D) + NORM_EPS)
            for c in range(NC):
                xv = src[c, rows, :].astype(F32)
                dst[rows, CH * c:CH * (c + 1)] = (xv * inv * gains[c]).astype(BF)
        return 0

    lax.fori_loop(0, ROWS // 128, block, 0)


def rope(y, tab, base):
    rows = []
    for s in range(2):
        cols = []
        for j in range(CH // 128):
            v = y[128 * s:128 * (s + 1), 128 * j:128 * (j + 1)]
            cols.append(v * tab[base] + pltpu.roll(v, 96, 1) * tab[base + 1] + pltpu.roll(v, 32, 1) * tab[base + 2])
        rows.append(jnp.concatenate(cols, axis=1))
    return jnp.concatenate(rows, axis=0)


def attend_probs(q, k, ch, pair, seq, lo, causal):
    rows, cols = pl.ds(128 * seq, 128), pl.ds(128 * pair, 128)
    qp, kp = q[ch, rows, cols], k[ch, rows, cols]
    zero = jnp.zeros((128, 128), BF)
    both = jnp.concatenate([jnp.where(lo, kp, zero), jnp.where(lo, zero, kp)], axis=0)
    scores = dott(qp, both)
    probs = []
    for head in range(2):
        z = jnp.where(causal, scores[:, 128 * head:128 * (head + 1)], -1e30)
        e = jnp.exp(z - jnp.max(z, axis=1, keepdims=True))
        probs.append((e * (1.0 / jnp.sum(e, axis=1, keepdims=True))).astype(BF))
    return jnp.concatenate(probs, axis=1)


def attend_values(q, v, ch, pair, seq, lo, probs):
    rows, cols = pl.ds(128 * seq, 128), pl.ds(128 * pair, 128)
    vp = v[ch, rows, cols]
    zero = jnp.zeros((128, 128), BF)
    both = jnp.concatenate([jnp.where(lo, vp, zero), jnp.where(lo, zero, vp)], axis=0)
    q[ch, rows, cols] = dotf(probs, both).astype(BF)


def kernel(x_hbm, emb, gf, tgt, ga, gm, wq, wk, wv, wo, wg, wu, wd, tab, flag, out, out_mean, xbuf,
           ring, res, xin, xfin, x1, h, q, k, v, a, xout, st, stf,
           wsem, rsem, xsem, recv_sem, send_sem, send0_sem, free_sem, free0_sem,
           fsend_sem, frecv_sem, ffwd_sem, ssend_sem, srecv_sem, tsend_sem, trecv_sem, gsend_sem, grecv_sem):
    me = lax.axis_index("pp")
    is_layer = jnp.logical_and(me >= FIRST, me <= LAST)
    is_head = jnp.logical_or(me == 0, me == 7)
    lane = lax.broadcasted_iota(jnp.int32, (128, 128), 1)
    lo = lane < 64
    causal = lax.broadcasted_iota(jnp.int32, (128, 128), 0) >= lane
    units = [(p, s) for p in range(4) for s in range(2)]

    def al(i, n):
        return i if isinstance(i, int) else pl.multiple_of(i, n)

    def slot_of(m, b):
        return lax.rem(BODIES * m + b, NG)

    def load(src, slot, t):
        pltpu.make_async_copy(src, ring.at[slot, t], wsem.at[slot]).start()

    def load_res(src, i):
        pltpu.make_async_copy(src, res.at[i], rsem.at[i]).start()

    def wait_group(slot):
        pltpu.make_async_copy(ring.at[slot], ring.at[slot], wsem.at[slot]).wait()

    def wait_res(i):
        pltpu.make_async_copy(res.at[i], res.at[i], rsem.at[i]).wait()

    def cols_of(w, c):
        return w.at[:, pl.ds(al(c * CH, CH), CH)]

    def start_qkv(i, slot):
        for t, w in enumerate((wq, wk, wv)):
            load(cols_of(w, i), slot, t)

    def start_out(slot):
        for t in range(3):
            load(cols_of(wo, t), slot, t)

    def start_ffn(c, slot):
        load(cols_of(wg, 2 * c), slot, 0)
        load(cols_of(wg, 2 * c + 1), slot, 1)
        load(cols_of(wu, 2 * c), slot, 2)

    def down_tile(n, t):
        return wd.at[pl.ds(D * t, D), pl.ds(al(n * CH, CH), CH)]

    def start_down(n, slot):
        for t in range(3):
            load(down_tile(n, t), slot, t)

    def to_next(s, n):
        return pltpu.make_async_remote_copy(xout.at[s, n], xin.at[s, n], send_sem.at[s, n], recv_sem.at[s, n],
                                            device_id={"pp": lax.rem(me + 1, 8)}, device_id_type=MESH)

    def to_zero(s, n):
        return pltpu.make_async_remote_copy(xout.at[s, n], xin.at[s, n], send0_sem.at[s, n], recv_sem.at[s, n],
                                            device_id={"pp": 0}, device_id_type=MESH)

    fin_targets = (7, 4, 2)

    def to_fin(i, s, n):
        return pltpu.make_async_remote_copy(xout.at[s, n], xfin.at[n], fsend_sem.at[i, n], frecv_sem.at[n],
                                            device_id={"pp": fin_targets[i]}, device_id_type=MESH)

    def forward(n):
        return pltpu.make_async_remote_copy(xfin.at[n], xfin.at[n], ffwd_sem.at[n], frecv_sem.at[n],
                                            device_id={"pp": lax.rem(me + 1, 8)}, device_id_type=MESH)

    pair = jnp.where(me == 0, 1, me)

    def to_first():
        return pltpu.make_async_remote_copy(x_hbm, xbuf.at[pair], gsend_sem, grecv_sem.at[pair],
                                            device_id={"pp": FIRST}, device_id_type=MESH)

    def start_x(m, s):
        cols = [pl.ds(CH * c, CH) for c in range(NC)]

        @pl.when(m < 2)
        def _():
            for c in range(NC):
                pltpu.make_async_copy(x_hbm.at[m, :, cols[c]], xin.at[s, c], xsem.at[s]).start()

        @pl.when(m >= 2)
        def _():
            p = m // 2

            @pl.when(m == 2 * p)
            def _():
                pltpu.make_async_copy(xbuf.at[p], xbuf.at[p], grecv_sem.at[p]).wait()

            for c in range(NC):
                pltpu.make_async_copy(xbuf.at[p, m - 2 * p, :, cols[c]], xin.at[s, c], xsem.at[s]).start()

    def wait_x(s):
        pltpu.make_async_copy(xin.at[s], xin.at[s], xsem.at[s]).wait()

    def start_head(row, slot):
        for t in range(4):
            pltpu.make_async_copy(emb.at[pl.ds(al(row, HG), HG), pl.ds(CH * t, CH)], res.at[4 * slot + t], rsem.at[slot]).start()

    def wait_head(slot):
        view = res.at[pl.ds(4 * slot, 4)]
        pltpu.make_async_copy(view, view, rsem.at[slot]).wait()

    sub8 = lax.broadcasted_iota(jnp.int32, (8, ROWS), 0)

    def head_group(slot, row, y, carry):
        mx, sm, pk = carry
        yrel = y - row - sub8
        for nb in range(HG // CH):
            lg = None
            for t in range(4):
                part = dott(res[4 * slot + t, CH * nb:CH * (nb + 1), :], h[:, CH * t:CH * (t + 1)])
                lg = part if lg is None else lg + part
            l3 = lg.reshape(CH // 8, 8, ROWS)
            new = jnp.maximum(mx, jnp.max(l3, axis=0))
            sm = sm * jnp.exp(mx - new) + jnp.sum(jnp.exp(l3 - new[None]), axis=0)
            for r in range(CH // 8):
                pk = pk + jnp.where(yrel == CH * nb + 8 * r, l3[r], 0.0)
            mx = new
        return mx, sm, pk

    def head_start():
        return (jnp.full((8, ROWS), -3e38, F32), jnp.zeros((8, ROWS), F32), jnp.zeros((8, ROWS), F32))

    def head_stats(carry):
        mx, sm, pk = carry
        top = jnp.max(mx, axis=0, keepdims=True)
        tot = jnp.sum(sm * jnp.exp(mx - top), axis=0, keepdims=True)
        return top, tot, jnp.sum(pk, axis=0, keepdims=True)

    @pl.when(me != FIRST)
    def _():
        to_first().start()

    @pl.when(is_layer)
    def _():
        @pl.when(me == FIRST)
        def _():
            start_x(0, 0)

        for i in range(3):
            start_qkv(i, i)

        @pl.when(me != FIRST)
        def _():
            load_res(cols_of(wo, 3), 0)
            for c in range(8):
                load_res(cols_of(wu, 2 * c + 1), 1 + c)
            for n in range(NC):
                load_res(down_tile(n, 3), 9 + n)

        def one(m, _):
            s = lax.rem(m, 2)
            first = m == 0
            fresh = jnp.logical_and(first, me == FIRST)
            more = m < NMB - 1

            @pl.when(me == FIRST)
            def _():
                wait_x(s)

                @pl.when(more)
                def _():
                    start_x(m + 1, 1 - s)

            @pl.when(me != FIRST)
            def _():
                for c in range(NC):
                    to_next(s, c).wait_recv()

            norm_rows(xin.at[s], ga, h)
            on = flag[0:1, 0:1] != 0

            def qkv(i, prev):
                slot = slot_of(m, i)
                wait_group(slot)
                us = units if prev is not None else []
                ps = [attend_probs(q, k, prev, p, sq, lo, causal) for p, sq in us]
                for j, dst in enumerate((q, k, v)):
                    r = dotf(h[...], ring[slot, j])
                    if j < 2:
                        r = rope(r, tab, 3 * j)
                    dst[i] = r.astype(BF)
                    for (p, sq), pr in zip(us, ps) if j == 1 else ():
                        attend_values(q, v, prev, p, sq, lo, pr)
                return slot

            slot = qkv(0, None)
            start_qkv(3, slot)

            def qkv_static(i):
                slot = qkv(i, i - 1)
                if i == 1:
                    start_out(slot)

                    @pl.when(fresh)
                    def _():
                        load_res(cols_of(wo, 3), 0)
                else:
                    start_ffn(i - 2, slot)

                    @pl.when(fresh)
                    def _():
                        load_res(cols_of(wu, 2 * (i - 2) + 1), 1 + i - 2)

            def qkv_loop(i, _):
                slot = qkv(i, i - 1)

                @pl.when(i == 1)
                def _():
                    start_out(slot)

                    @pl.when(fresh)
                    def _():
                        load_res(cols_of(wo, 3), 0)

                @pl.when(i > 1)
                def _():
                    start_ffn(i - 2, slot)

                    @pl.when(fresh)
                    def _():
                        load_res(cols_of(wu, 2 * (i - 2) + 1), 1 + i - 2)
                return 0

            for i in range(1, 4):
                qkv_static(i)
            slot = slot_of(m, 4)
            wait_group(slot)

            @pl.when(first)
            def _():
                wait_res(0)

            def out_tile(t):
                return ring.at[slot, t] if t < 3 else res.at[0]

            def out_part(t):
                w, r = out_tile(t), None
                for kc in range(NC - 1):
                    part = dotf(q[kc], w[CH * kc:CH * (kc + 1), :])
                    r = part if r is None else r + part
                return r

            ps = [attend_probs(q, k, 3, p, sq, lo, causal) for p, sq in units]
            done = [out_part(t) for t in range(2)]
            for (p, sq), pr in zip(units, ps):
                attend_values(q, v, 3, p, sq, lo, pr)
            done += [out_part(t) for t in range(2, NC)]
            for t in range(NC):
                r = done[t] + dotf(q[3], out_tile(t)[CH * 3:, :])
                xo = xin[s, t]
                x1[t] = jnp.where(on, (xo.astype(F32) + r).astype(BF), xo)
            start_ffn(2, slot)

            @pl.when(fresh)
            def _():
                load_res(cols_of(wu, 2 * 2 + 1), 1 + 2)

            @pl.when(jnp.logical_and(me != FIRST, m < NMB - 2))
            def _():
                pl.semaphore_signal(free_sem, 1, device_id={"pp": lax.rem(me + 7, 8)}, device_id_type=MESH)

            norm_rows(x1, gm, h)

            def ffn2(i, _):
                for e in range(4):
                    ffn(4 * i + e, 0)
                return 0

            def ffn(c, _):
                slot = slot_of(m, 5 + c)
                wait_group(slot)

                @pl.when(first)
                def _():
                    wait_res(1 + c)

                for t in range(2):
                    gate = dotf(h[...], ring[slot, t])
                    up = dotf(h[...], ring[slot, 2] if t == 0 else res[1 + c])
                    a[c, :, CH * t:CH * (t + 1)] = (gate * (1.0 / (1.0 + jnp.exp(-gate))) * up).astype(BF)

                @pl.when(c < 5)
                def _():
                    start_ffn(c + 3, slot)

                    @pl.when(fresh)
                    def _():
                        load_res(cols_of(wu, 2 * (c + 3) + 1), 1 + c + 3)

                @pl.when(c >= 5)
                def _():
                    start_down(c - 5, slot)

                    @pl.when(fresh)
                    def _():
                        load_res(down_tile(c - 5, 3), 9 + c - 5)
                return 0

            lax.fori_loop(0, 2, ffn2, 0)

            @pl.when(jnp.logical_and(m >= 2, jnp.logical_or(more, me != LAST)))
            def _():
                pl.semaphore_wait(free_sem, 1)

                @pl.when(me == LAST)
                def _():
                    pl.semaphore_wait(free0_sem, 1)

            def down(n, _):
                slot = slot_of(m, 13 + n)
                wait_group(slot)

                @pl.when(first)
                def _():
                    wait_res(9 + n)

                @pl.when(m >= 2)
                def _():
                    to_next(s, n).wait_send()

                    @pl.when(me == LAST)
                    def _():
                        to_zero(s, n).wait_send()

                acc = None
                for t in range(4):
                    w = ring.at[slot, t] if t < 3 else res.at[9 + n]
                    for u in range(2):
                        part = dotf(a[2 * t + u], w[1024 * u:1024 * (u + 1), :])
                        acc = part if acc is None else acc + part
                xo = x1[n]
                xout[s, n] = jnp.where(on, (xo.astype(F32) + acc).astype(BF), xo)

                @pl.when(jnp.logical_or(more, me != LAST))
                def _():
                    to_next(s, n).start()

                @pl.when(me == LAST)
                def _():
                    @pl.when(more)
                    def _():
                        to_zero(s, n).start()

                    @pl.when(jnp.logical_not(more))
                    def _():
                        for i in range(3):
                            to_fin(i, s, n).start()

                if n == 0:
                    start_down(3, slot)

                    @pl.when(fresh)
                    def _():
                        load_res(down_tile(3, 3), 12)
                else:
                    @pl.when(more)
                    def _():
                        start_qkv(n - 1, slot)
                return 0

            for n in range(NC):
                down(n, 0)
            return 0

        lax.fori_loop(0, NMB, one, 0)

    side = jnp.where(me == 7, 1, 0)
    base = side * (VOCAB // 2)

    def stats_to(i):
        return pltpu.make_async_remote_copy(st.at[side], st.at[side], ssend_sem.at[i], srecv_sem.at[side],
                                            device_id={"pp": lax.rem(me + 1 + i, 8)}, device_id_type=MESH)

    @pl.when(is_head)
    def _():
        for g in range(3):
            start_head(base + HG * g, g)

        def one(m, _):
            s = lax.rem(m, 2)
            for c in range(NC):
                to_next(s, c).wait_recv()
            norm_rows(xin.at[s], gf, h)

            @pl.when(m < NMB - 3)
            def _():
                @pl.when(me == 7)
                def _():
                    pl.semaphore_signal(free_sem, 1, device_id={"pp": LAST}, device_id_type=MESH)

                @pl.when(me == 0)
                def _():
                    pl.semaphore_signal(free0_sem, 1, device_id={"pp": LAST}, device_id_type=MESH)

            y = tgt[pl.ds(m, 1), :]

            def group(g, carry):
                slot = lax.rem(g, 3)
                wait_head(slot)
                row = base + HG * g
                carry = head_group(slot, row, y, carry)

                @pl.when(g < HEAD_GROUPS - 3)
                def _():
                    start_head(row + 3 * HG, slot)

                @pl.when(jnp.logical_and(g >= HEAD_GROUPS - 3, m < NMB - 2))
                def _():
                    start_head(row + 3 * HG - HG * HEAD_GROUPS, slot)
                return carry

            top, tot, pick = head_stats(lax.fori_loop(0, HEAD_GROUPS, group, head_start()))
            st[side, 0, pl.ds(m, 1), :] = top
            st[side, 1, pl.ds(m, 1), :] = tot
            st[side, 2, pl.ds(m, 1), :] = pick
            return 0

        lax.fori_loop(0, NMB - 1, one, 0)
        for j in range(3):
            st[side, j, NMB - 1:NMB, :] = jnp.ones((1, ROWS), F32)
        for i in range(7):
            stats_to(i).start()

    part = me - 2

    def fin_to(i):
        return pltpu.make_async_remote_copy(stf.at[part], stf.at[part], tsend_sem.at[i], trecv_sem.at[part],
                                            device_id={"pp": lax.rem(me + 1 + i, 8)}, device_id_type=MESH)

    @pl.when(me >= 2)
    def _():
        row0 = part * (HG * FIN_GROUPS)
        for g in range(3):
            start_head(row0 + HG * g, g)

        @pl.when(me == LAST)
        def _():
            for n in range(NC):
                xfin[n] = xout[(NMB - 1) % 2, n]

        @pl.when(me != LAST)
        def _():
            for n in range(NC):
                forward(n).wait_recv()

                @pl.when(jnp.logical_or(me == 2, me == 4))
                def _():
                    forward(n).start()

        norm_rows(xfin, gf, h)
        y = tgt[NMB - 1:NMB, :]

        def group(g, carry):
            slot = lax.rem(g, 3)
            wait_head(slot)
            row = row0 + HG * g
            carry = head_group(slot, row, y, carry)

            @pl.when(g < FIN_GROUPS - 3)
            def _():
                start_head(row + 3 * HG, slot)
            return carry

        top, tot, pick = head_stats(lax.fori_loop(0, FIN_GROUPS, group, head_start()))
        stf[part] = jnp.concatenate([top, tot, pick, jnp.zeros((5, ROWS), F32)], axis=0)
        for i in range(7):
            fin_to(i).start()

    for d in range(2):
        @pl.when(me != 7 * d)
        def _():
            pltpu.make_async_copy(st.at[d], st.at[d], srecv_sem.at[d]).wait()
    for f in range(6):
        @pl.when(me != f + 2)
        def _():
            pltpu.make_async_copy(stf.at[f], stf.at[f], trecv_sem.at[f]).wait()

    top = jnp.maximum(st[0, 0], st[1, 0])
    tot = st[0, 1] * jnp.exp(st[0, 0] - top) + st[1, 1] * jnp.exp(st[1, 0] - top)
    loss = jnp.log(tot) + top - (st[0, 2] + st[1, 2])
    ftop = stf[0, 0:1, :]
    for f in range(1, 6):
        ftop = jnp.maximum(ftop, stf[f, 0:1, :])
    ftot = jnp.zeros((1, ROWS), F32)
    fpick = jnp.zeros((1, ROWS), F32)
    for f in range(6):
        ftot = ftot + stf[f, 1:2, :] * jnp.exp(stf[f, 0:1, :] - ftop)
        fpick = fpick + stf[f, 2:3, :]
    last = lax.broadcasted_iota(jnp.int32, (NMB, ROWS), 0) == NMB - 1
    loss = jnp.where(last, jnp.log(ftot) + ftop - fpick, loss)
    out[:, 0, :] = loss[:, :128]
    out[:, 1, :] = loss[:, 128:]
    mean = jnp.sum(loss, axis=1, keepdims=True) * (1.0 / ROWS)
    here = lax.broadcasted_iota(jnp.int32, (NMB, 128), 0) == lax.broadcasted_iota(jnp.int32, (NMB, 128), 1)
    out_mean[...] = jnp.sum(jnp.where(here, mean, 0.0), axis=0, keepdims=True)

    @pl.when(me != FIRST)
    def _():
        to_first().wait_send()

    @pl.when(is_layer)
    def _():
        for n in range(NC):
            to_next(0, n).wait_send()

            @pl.when(me != LAST)
            def _():
                to_next(1, n).wait_send()

            @pl.when(me == LAST)
            def _():
                to_zero(0, n).wait_send()
                for i in range(3):
                    to_fin(i, 1, n).wait_send()

    @pl.when(is_head)
    def _():
        for i in range(7):
            stats_to(i).wait_send()

    @pl.when(me >= 2)
    def _():
        for i in range(7):
            fin_to(i).wait_send()

        @pl.when(jnp.logical_or(me == 2, me == 4))
        def _():
            for n in range(NC):
                forward(n).wait_send()


def run_kernel(*args):
    hbm = pl.BlockSpec(memory_space=pltpu.HBM)
    vmem = pl.BlockSpec(memory_space=pltpu.VMEM)
    dma, regular = pltpu.SemaphoreType.DMA, pltpu.SemaphoreType.REGULAR
    return pl.pallas_call(
        kernel,
        out_shape=(jax.ShapeDtypeStruct((NMB, 2, 128), F32), jax.ShapeDtypeStruct((1, 128), F32),
                   jax.ShapeDtypeStruct((NMB // 2, 2, ROWS, D), BF)),
        in_specs=[hbm, hbm, vmem, vmem, vmem, vmem] + [hbm] * 7 + [vmem, vmem],
        out_specs=(vmem, vmem, hbm),
        scratch_shapes=[
            pltpu.VMEM((NG, 3, D, CH), BF),
            pltpu.VMEM((13, D, CH), BF),
            pltpu.VMEM((2, NC, ROWS, CH), BF),
            pltpu.VMEM((NC, ROWS, CH), BF),
            pltpu.VMEM((NC, ROWS, CH), BF),
            pltpu.VMEM((ROWS, D), BF),
            pltpu.VMEM((NC, ROWS, CH), BF),
            pltpu.VMEM((NC, ROWS, CH), BF),
            pltpu.VMEM((NC, ROWS, CH), BF),
            pltpu.VMEM((8, ROWS, 1024), BF),
            pltpu.VMEM((2, NC, ROWS, CH), BF),
            pltpu.VMEM((2, 3, NMB, ROWS), F32),
            pltpu.VMEM((6, 8, ROWS), F32),
            dma((NG,)), dma((13,)), dma((2,)), dma((2, NC)), dma((2, NC)), dma((2, NC)), regular, regular,
            dma((3, NC)), dma((NC,)), dma((NC,)), dma((7,)), dma((2,)), dma((7,)), dma((6,)), dma(()), dma((8,)),
        ],
        compiler_params=pltpu.CompilerParams(vmem_limit_bytes=67043328, has_side_effects=True),
    )(*args)


def solution(mesh):
    def stage_program(tokens, targets, emb, g_final, active, g_attn, w_q, w_k, w_v, w_o, g_mlp, w_gate, w_up, w_down):
        me = lax.axis_index("pp")
        pair = jnp.where(me == FIRST, 0, jnp.where(me == 0, 1, me))
        ids = lax.dynamic_slice_in_dim(tokens.reshape(NMB, ROWS), 2 * pair, 2, axis=0)
        x = emb.at[ids.reshape(2 * ROWS)].get(mode="promise_in_bounds").reshape(2, ROWS, D)
        flag = jnp.broadcast_to(active.reshape(1, 1), (8, 128))
        token_loss, mean, _ = run_kernel(x, emb, g_final.reshape(1, D), targets.reshape(NMB, ROWS), g_attn.reshape(1, D), g_mlp.reshape(1, D),
          w_q.reshape(D, D), w_k.reshape(D, D), w_v.reshape(D, D), w_o.reshape(D, D),
          w_gate.reshape(D, FFN), w_up.reshape(D, FFN), w_down.reshape(FFN, D), rope_tables(), flag)
        return token_loss, mean[0, :NMB]

    stack = P("pp")
    in_specs = (P("dp"), P("dp"), P(), P()) + (stack,) * 10
    return jax.shard_map(stage_program, mesh=mesh, in_specs=in_specs, out_specs=(P("dp"), P("dp")), check_vma=False)
```

```python
import functools
import math

import jax
import jax.numpy as jnp
import numpy as np
from jax import lax
from jax.experimental import pallas as pl
from jax.experimental.pallas import tpu as pltpu
from jax.sharding import PartitionSpec as P

BF = jnp.bfloat16
F32 = jnp.float32
NORM_EPS = 1e-5
ROPE_BASE = 500000.0
ROPE_FACTOR = 32.0
ROPE_LOW = 1.0
ROPE_HIGH = 4.0
ROPE_ORIG = 8192.0

NMB = 16
ROWS = 256
D = 2048
FFN = 8192
VOCAB = 49152
CH = 512
NC = D // CH
NG = 4
BODIES = 17
FIRST, LAST = 1, 6
HG = 2048
HEAD_GROUPS = VOCAB // 2 // HG
FIN_GROUPS = VOCAB // 6 // HG
MESH = pl.DeviceIdType.MESH


def rope_tables():
    half = 32
    inv_freq = ROPE_BASE ** (-2.0 * np.arange(half) / (2 * half))
    wavelen = 2.0 * math.pi / inv_freq
    smooth = np.clip((ROPE_ORIG / wavelen - ROPE_LOW) / (ROPE_HIGH - ROPE_LOW), 0.0, 1.0)
    scaled = (1.0 - smooth) * inv_freq / ROPE_FACTOR + smooth * inv_freq
    angles = np.arange(128)[:, None] * scaled[None, :]
    c, s = np.cos(angles), np.sin(angles)
    z = np.zeros_like(s)
    t = np.stack([np.tile(c, (1, 4)), np.tile(np.concatenate([-s, z], 1), (1, 2)), np.tile(np.concatenate([z, s], 1), (1, 2))])
    return np.concatenate([t * 0.125, t], 0).astype(np.float32)


def dotf(a, b):
    return jnp.dot(a, b, preferred_element_type=F32)


def dott(a, b):
    return lax.dot_general(a, b, (((1,), (1,)), ((), ())), preferred_element_type=F32)


def norm_rows(src, g_ref, dst):
    gains = [g_ref[0:1, CH * c:CH * (c + 1)].astype(F32) for c in range(NC)]

    def block(i, _):
        r0 = pl.multiple_of(i * 256, 256)
        for u in range(16):
            rows = pl.ds(r0 + 16 * u, 16)
            ss = None
            for c in range(NC):
                xv = src[c, rows, :].astype(F32)
                sq = xv * xv
                part = sq[:, :128] + sq[:, 128:256] + sq[:, 256:384] + sq[:, 384:]
                ss = part if ss is None else ss + part
            inv = lax.rsqrt(jnp.sum(ss, axis=1, keepdims=True) * (1.0 / D) + NORM_EPS)
            for c in range(NC):
                xv = src[c, rows, :].astype(F32)
                dst[rows, CH * c:CH * (c + 1)] = (xv * inv * gains[c]).astype(BF)
        return 0

    lax.fori_loop(0, ROWS // 256, block, 0)


def rope(y, tab, base):
    rows = []
    for s in range(2):
        cols = []
        for j in range(CH // 128):
            v = y[128 * s:128 * (s + 1), 128 * j:128 * (j + 1)]
            cols.append(v * tab[base] + pltpu.roll(v, 96, 1) * tab[base + 1] + pltpu.roll(v, 32, 1) * tab[base + 2])
        rows.append(jnp.concatenate(cols, axis=1))
    return jnp.concatenate(rows, axis=0)


def attend_probs(q, k, ch, pair, seq, lo, causal):
    rows, cols = pl.ds(128 * seq, 128), pl.ds(128 * pair, 128)
    qp, kp = q[ch, rows, cols], k[rows, pl.ds(CH * (ch % 2) + 128 * pair, 128)]
    zero = jnp.zeros((128, 128), BF)
    both = jnp.concatenate([jnp.where(lo, kp, zero), jnp.where(lo, zero, kp)], axis=0)
    scores = dott(qp, both)
    probs = []
    for head in range(2):
        z = jnp.where(causal, scores[:, 128 * head:128 * (head + 1)], -1e30)
        e = jnp.exp(z - jnp.max(z, axis=1, keepdims=True))
        probs.append((e * (1.0 / jnp.sum(e, axis=1, keepdims=True))).astype(BF))
    return jnp.concatenate(probs, axis=1)


def attend_values(q, v, ch, pair, seq, lo, probs):
    rows, cols = pl.ds(128 * seq, 128), pl.ds(128 * pair, 128)
    vp = v[rows, pl.ds(CH * (ch % 2) + 128 * pair, 128)]
    zero = jnp.zeros((128, 128), BF)
    both = jnp.concatenate([jnp.where(lo, vp, zero), jnp.where(lo, zero, vp)], axis=0)
    q[ch, rows, cols] = dotf(probs, both).astype(BF)


def kernel(x_hbm, emb, gf, tgt, ga, gm, wq, wk, wv, wo, wg, wu, wd, tab, flag, out, out_mean, xbuf,
           ring, res, xin, xfin, h, q, a, xout, st, stf,
           wsem, rsem, xsem, recv_sem, send_sem, send0_sem, free_sem, free0_sem,
           fsend_sem, frecv_sem, ffwd_sem, ssend_sem, srecv_sem, tsend_sem, trecv_sem, gsend_sem, grecv_sem):
    me = lax.axis_index("pp")
    k, v = a.at[0], a.at[1]
    is_layer = jnp.logical_and(me >= FIRST, me <= LAST)
    is_head = jnp.logical_or(me == 0, me == 7)
    lane = lax.broadcasted_iota(jnp.int32, (128, 128), 1)
    lo = lane < 64
    causal = lax.broadcasted_iota(jnp.int32, (128, 128), 0) >= lane
    units = [(p, s) for p in range(4) for s in range(2)]

    def al(i, n):
        return i if isinstance(i, int) else pl.multiple_of(i, n)

    def slot_of(m, b):
        return lax.rem(BODIES * m + b, NG)

    def load(src, slot, t):
        pltpu.make_async_copy(src, ring.at[slot, t], wsem.at[slot]).start()

    def load_res(src, i):
        pltpu.make_async_copy(src, res.at[i], rsem.at[i]).start()

    def wait_group(slot):
        pltpu.make_async_copy(ring.at[slot], ring.at[slot], wsem.at[slot]).wait()

    def wait_res(i):
        pltpu.make_async_copy(res.at[i], res.at[i], rsem.at[i]).wait()

    def cols_of(w, c):
        return w.at[:, pl.ds(al(c * CH, CH), CH)]

    def start_qkv(i, slot):
        for t, w in enumerate((wq, wk, wv)):
            load(cols_of(w, i), slot, t)

    def start_out(slot):
        for t in range(3):
            load(cols_of(wo, t), slot, t)

    def start_ffn(c, slot):
        load(cols_of(wg, 2 * c), slot, 0)
        load(cols_of(wg, 2 * c + 1), slot, 1)
        load(cols_of(wu, 2 * c), slot, 2)

    def down_tile(n, t):
        return wd.at[pl.ds(D * t, D), pl.ds(al(n * CH, CH), CH)]

    def start_down(n, slot):
        for t in range(3):
            load(down_tile(n, t), slot, t)

    def to_next(s, n):
        return pltpu.make_async_remote_copy(xout.at[n], xin.at[s, n], send_sem.at[n], recv_sem.at[s, n],
                                            device_id={"pp": lax.rem(me + 1, 8)}, device_id_type=MESH)

    def to_zero(s, n):
        return pltpu.make_async_remote_copy(xout.at[n], xin.at[s, n], send0_sem.at[n], recv_sem.at[s, n],
                                            device_id={"pp": 0}, device_id_type=MESH)

    fin_targets = (7, 4, 2)

    def to_fin(i, s, n):
        return pltpu.make_async_remote_copy(xout.at[n], xfin.at[n], fsend_sem.at[i, n], frecv_sem.at[n],
                                            device_id={"pp": fin_targets[i]}, device_id_type=MESH)

    def forward(n):
        return pltpu.make_async_remote_copy(xfin.at[n], xfin.at[n], ffwd_sem.at[n], frecv_sem.at[n],
                                            device_id={"pp": lax.rem(me + 1, 8)}, device_id_type=MESH)

    pair = jnp.where(me == 0, 1, me)

    def to_first():
        return pltpu.make_async_remote_copy(x_hbm, xbuf.at[pair], gsend_sem, grecv_sem.at[pair],
                                            device_id={"pp": FIRST}, device_id_type=MESH)

    def start_x(m, s):
        cols = [pl.ds(CH * c, CH) for c in range(NC)]

        @pl.when(m < 2)
        def _():
            for c in range(NC):
                pltpu.make_async_copy(x_hbm.at[m, :, cols[c]], xin.at[s, c], xsem.at[s]).start()

        @pl.when(m >= 2)
        def _():
            p = m // 2

            @pl.when(m == 2 * p)
            def _():
                pltpu.make_async_copy(xbuf.at[p], xbuf.at[p], grecv_sem.at[p]).wait()

            for c in range(NC):
                pltpu.make_async_copy(xbuf.at[p, m - 2 * p, :, cols[c]], xin.at[s, c], xsem.at[s]).start()

    def wait_x(s):
        pltpu.make_async_copy(xin.at[s], xin.at[s], xsem.at[s]).wait()

    def start_head(row, slot):
        for t in range(4):
            pltpu.make_async_copy(emb.at[pl.ds(al(row, HG), HG), pl.ds(CH * t, CH)], res.at[4 * slot + t], rsem.at[slot]).start()

    def wait_head(slot):
        view = res.at[pl.ds(4 * slot, 4)]
        pltpu.make_async_copy(view, view, rsem.at[slot]).wait()

    sub8 = lax.broadcasted_iota(jnp.int32, (8, ROWS), 0)

    def head_group(slot, row, y, carry):
        mx, sm, pk = carry
        yrel = y - row - sub8
        for nb in range(HG // CH):
            lg = None
            for t in range(4):
                part = dott(res[4 * slot + t, CH * nb:CH * (nb + 1), :], h[:, CH * t:CH * (t + 1)])
                lg = part if lg is None else lg + part
            l3 = lg.reshape(CH // 8, 8, ROWS)
            new = jnp.maximum(mx, jnp.max(l3, axis=0))
            sm = sm * jnp.exp(mx - new) + jnp.sum(jnp.exp(l3 - new[None]), axis=0)
            for r in range(CH // 8):
                pk = pk + jnp.where(yrel == CH * nb + 8 * r, l3[r], 0.0)
            mx = new
        return mx, sm, pk

    def target_row(m):
        return jnp.concatenate([tgt[m, 0:1, :], tgt[m, 1:2, :]], axis=1)

    def head_start():
        return (jnp.full((8, ROWS), -3e38, F32), jnp.zeros((8, ROWS), F32), jnp.zeros((8, ROWS), F32))

    def head_stats(carry):
        mx, sm, pk = carry
        top = jnp.max(mx, axis=0, keepdims=True)
        tot = jnp.sum(sm * jnp.exp(mx - top), axis=0, keepdims=True)
        return top, tot, jnp.sum(pk, axis=0, keepdims=True)

    @pl.when(me != FIRST)
    def _():
        to_first().start()

    @pl.when(is_layer)
    def _():
        @pl.when(me == FIRST)
        def _():
            start_x(0, 0)

        for i in range(2):
            start_qkv(i, i)

        @pl.when(me != FIRST)
        def _():
            for i in range(2, NG):
                start_qkv(i, i)
            load_res(cols_of(wo, 3), 0)
            for c in range(8):
                load_res(cols_of(wu, 2 * c + 1), 1 + c)
            for n in range(NC):
                load_res(down_tile(n, 3), 9 + n)

        def one(m, _):
            s = lax.rem(m, 2)
            first = m == 0
            fresh = jnp.logical_and(first, me == FIRST)
            more = m < NMB - 1

            @pl.when(me == FIRST)
            def _():
                wait_x(s)

                @pl.when(more)
                def _():
                    start_x(m + 1, 1 - s)

            @pl.when(me != FIRST)
            def _():
                for c in range(NC):
                    to_next(s, c).wait_recv()

            norm_rows(xin.at[s], ga, h)
            on = flag[0:1, 0:1] != 0

            def begin(*bodies):
                for b in bodies:
                    wait_group(slot_of(m, b))

            def begin_res(*tiles):
                @pl.when(first)
                def _():
                    for i in tiles:
                        wait_res(i)

            def start_body(b, slot):
                if b < 4:
                    start_qkv(b, slot)
                elif b == 4:
                    start_out(slot)
                elif b < 13:
                    start_ffn(b - 5, slot)
                else:
                    start_down(b - 13, slot)

            def refill(b):
                slot, later = slot_of(m, b), b + NG
                if later < BODIES:
                    start_body(later, slot)

                    @pl.when(fresh)
                    def _():
                        if later == 4:
                            load_res(cols_of(wo, 3), 0)
                        elif later < 13:
                            load_res(cols_of(wu, 2 * (later - 5) + 1), 1 + later - 5)
                        else:
                            load_res(down_tile(later - 13, 3), 9 + later - 13)
                else:
                    @pl.when(more)
                    def _():
                        start_body(later - BODIES, slot)

            def qkv(i):
                slot = slot_of(m, i)
                us = units if i > 0 else []
                ps = [attend_probs(q, k, i - 1, p, sq, lo, causal) for p, sq in us]
                for j, dst in enumerate((q, k, v)):
                    r = dotf(h[...], ring[slot, j])
                    if j < 2:
                        r = rope(r, tab, 3 * j)
                    if j == 0:
                        q[i] = r.astype(BF)
                    else:
                        dst[:, CH * (i % 2):CH * (i % 2) + CH] = r.astype(BF)
                    for (p, sq), pr in zip(us, ps) if j == 1 else ():
                        attend_values(q, v, i - 1, p, sq, lo, pr)

            def ffn(c):
                slot = slot_of(m, 5 + c)
                for t in range(2):
                    gate = dotf(h[...], ring[slot, t])
                    up = dotf(h[...], ring[slot, 2] if t == 0 else res[1 + c])
                    a[c, :, CH * t:CH * (t + 1)] = (gate * (1.0 / (1.0 + jnp.exp(-gate))) * up).astype(BF)

            def down(n):
                slot = slot_of(m, 13 + n)
                acc = None
                for t in range(4):
                    w = ring.at[slot, t] if t < 3 else res.at[9 + n]
                    for u in range(2):
                        part = dotf(a[2 * t + u], w[1024 * u:1024 * (u + 1), :])
                        acc = part if acc is None else acc + part
                xo = xin[s, n]
                xout[n] = jnp.where(on, (xo.astype(F32) + acc).astype(BF), xo)

                @pl.when(jnp.logical_or(more, me != LAST))
                def _():
                    to_next(s, n).start()

                @pl.when(me == LAST)
                def _():
                    @pl.when(more)
                    def _():
                        to_zero(s, n).start()

                    @pl.when(jnp.logical_not(more))
                    def _():
                        for i in range(3):
                            to_fin(i, s, n).start()

            for i in (0, 2):
                begin(i, i + 1)

                @pl.when(jnp.logical_and(fresh, i == 0))
                def _():
                    for j in range(2, NG):
                        start_qkv(j, j)

                qkv(i)
                refill(i)
                qkv(i + 1)
                refill(i + 1)

            begin(4, 5)
            begin_res(0, 1)
            slot = slot_of(m, 4)

            def out_tile(t):
                return ring.at[slot, t] if t < 3 else res.at[0]

            def out_part(t):
                w, r = out_tile(t), None
                for kc in range(NC - 1):
                    part = dotf(q[kc], w[CH * kc:CH * (kc + 1), :])
                    r = part if r is None else r + part
                return r

            ps = [attend_probs(q, k, 3, p, sq, lo, causal) for p, sq in units]
            done = [out_part(t) for t in range(2)]
            for (p, sq), pr in zip(units, ps):
                attend_values(q, v, 3, p, sq, lo, pr)
            done += [out_part(t) for t in range(2, NC)]
            for t in range(NC):
                r = done[t] + dotf(q[3], out_tile(t)[CH * 3:, :])
                xo = xin[s, t]
                xin[s, t] = jnp.where(on, (xo.astype(F32) + r).astype(BF), xo)
            refill(4)
            norm_rows(xin.at[s], gm, h)
            ffn(0)
            refill(5)

            def ffn_pair(i, _):
                c = 1 + 2 * i
                begin(5 + c, 6 + c)
                begin_res(1 + c, 2 + c)
                ffn(c)
                ffn(c + 1)
                for e in range(3):
                    @pl.when(i == e)
                    def _():
                        refill(6 + 2 * e)
                        refill(7 + 2 * e)
                return 0

            lax.fori_loop(0, 3, ffn_pair, 0)

            @pl.when(jnp.logical_and(m >= 2, jnp.logical_or(more, me != LAST)))
            def _():
                pl.semaphore_wait(free_sem, 1)

                @pl.when(me == LAST)
                def _():
                    pl.semaphore_wait(free0_sem, 1)

            @pl.when(m >= 1)
            def _():
                for n in range(NC):
                    to_next(s, n).wait_send()

                    @pl.when(me == LAST)
                    def _():
                        to_zero(s, n).wait_send()

            begin(12, 13)
            begin_res(8, 9)
            ffn(7)
            refill(12)
            down(0)
            refill(13)
            begin(14, 15)
            begin_res(10, 11)
            down(1)
            refill(14)
            down(2)
            refill(15)
            begin(16)
            begin_res(12)
            down(3)
            refill(16)

            @pl.when(jnp.logical_and(me != FIRST, m < NMB - 2))
            def _():
                pl.semaphore_signal(free_sem, 1, device_id={"pp": lax.rem(me + 7, 8)}, device_id_type=MESH)
            return 0

        lax.fori_loop(0, NMB, one, 0)

    side = jnp.where(me == 7, 1, 0)
    base = side * (VOCAB // 2)

    def stats_to(i):
        return pltpu.make_async_remote_copy(st.at[side], st.at[side], ssend_sem.at[i], srecv_sem.at[side],
                                            device_id={"pp": lax.rem(me + 1 + i, 8)}, device_id_type=MESH)

    @pl.when(is_head)
    def _():
        for g in range(3):
            start_head(base + HG * g, g)

        def one(m, _):
            s = lax.rem(m, 2)
            for c in range(NC):
                to_next(s, c).wait_recv()
            norm_rows(xin.at[s], gf, h)

            @pl.when(m < NMB - 3)
            def _():
                @pl.when(me == 7)
                def _():
                    pl.semaphore_signal(free_sem, 1, device_id={"pp": LAST}, device_id_type=MESH)

                @pl.when(me == 0)
                def _():
                    pl.semaphore_signal(free0_sem, 1, device_id={"pp": LAST}, device_id_type=MESH)

            y = target_row(m)

            def group(g, carry):
                slot = lax.rem(g, 3)
                wait_head(slot)
                row = base + HG * g
                carry = head_group(slot, row, y, carry)

                @pl.when(g < HEAD_GROUPS - 3)
                def _():
                    start_head(row + 3 * HG, slot)

                @pl.when(jnp.logical_and(g >= HEAD_GROUPS - 3, m < NMB - 2))
                def _():
                    start_head(row + 3 * HG - HG * HEAD_GROUPS, slot)
                return carry

            top, tot, pick = head_stats(lax.fori_loop(0, HEAD_GROUPS, group, head_start()))
            st[side, 0, pl.ds(m, 1), :] = top
            st[side, 1, pl.ds(m, 1), :] = tot
            st[side, 2, pl.ds(m, 1), :] = pick
            return 0

        lax.fori_loop(0, NMB - 1, one, 0)
        for j in range(3):
            st[side, j, NMB - 1:NMB, :] = jnp.ones((1, ROWS), F32)
        for i in range(7):
            stats_to(i).start()

    part = me - 2

    def fin_to(i):
        return pltpu.make_async_remote_copy(stf.at[part], stf.at[part], tsend_sem.at[i], trecv_sem.at[part],
                                            device_id={"pp": lax.rem(me + 1 + i, 8)}, device_id_type=MESH)

    @pl.when(me >= 2)
    def _():
        row0 = part * (HG * FIN_GROUPS)
        for g in range(3):
            start_head(row0 + HG * g, g)

        @pl.when(me == LAST)
        def _():
            for n in range(NC):
                xfin[n] = xout[n]

        @pl.when(me != LAST)
        def _():
            for n in range(NC):
                forward(n).wait_recv()

                @pl.when(jnp.logical_or(me == 2, me == 4))
                def _():
                    forward(n).start()

        norm_rows(xfin, gf, h)
        y = target_row(NMB - 1)

        def group(g, carry):
            slot = lax.rem(g, 3)
            wait_head(slot)
            row = row0 + HG * g
            carry = head_group(slot, row, y, carry)

            @pl.when(g < FIN_GROUPS - 3)
            def _():
                start_head(row + 3 * HG, slot)
            return carry

        top, tot, pick = head_stats(lax.fori_loop(0, FIN_GROUPS, group, head_start()))
        stf[part] = jnp.concatenate([top, tot, pick, jnp.zeros((5, ROWS), F32)], axis=0)
        for i in range(7):
            fin_to(i).start()

    for d in range(2):
        @pl.when(me != 7 * d)
        def _():
            pltpu.make_async_copy(st.at[d], st.at[d], srecv_sem.at[d]).wait()
    for f in range(6):
        @pl.when(me != f + 2)
        def _():
            pltpu.make_async_copy(stf.at[f], stf.at[f], trecv_sem.at[f]).wait()

    top = jnp.maximum(st[0, 0], st[1, 0])
    tot = st[0, 1] * jnp.exp(st[0, 0] - top) + st[1, 1] * jnp.exp(st[1, 0] - top)
    loss = jnp.log(tot) + top - (st[0, 2] + st[1, 2])
    ftop = stf[0, 0:1, :]
    for f in range(1, 6):
        ftop = jnp.maximum(ftop, stf[f, 0:1, :])
    ftot = jnp.zeros((1, ROWS), F32)
    fpick = jnp.zeros((1, ROWS), F32)
    for f in range(6):
        ftot = ftot + stf[f, 1:2, :] * jnp.exp(stf[f, 0:1, :] - ftop)
        fpick = fpick + stf[f, 2:3, :]
    last = lax.broadcasted_iota(jnp.int32, (NMB, ROWS), 0) == NMB - 1
    loss = jnp.where(last, jnp.log(ftot) + ftop - fpick, loss)
    out[:, 0, :] = loss[:, :128]
    out[:, 1, :] = loss[:, 128:]
    mean = jnp.sum(loss, axis=1, keepdims=True) * (1.0 / ROWS)
    here = lax.broadcasted_iota(jnp.int32, (NMB, 128), 0) == lax.broadcasted_iota(jnp.int32, (NMB, 128), 1)
    out_mean[...] = jnp.sum(jnp.where(here, mean, 0.0), axis=0, keepdims=True)

    @pl.when(me != FIRST)
    def _():
        to_first().wait_send()

    @pl.when(is_layer)
    def _():
        for n in range(NC):
            @pl.when(me != LAST)
            def _():
                to_next(1, n).wait_send()

            @pl.when(me == LAST)
            def _():
                for i in range(3):
                    to_fin(i, 1, n).wait_send()

    @pl.when(is_head)
    def _():
        for i in range(7):
            stats_to(i).wait_send()

    @pl.when(me >= 2)
    def _():
        for i in range(7):
            fin_to(i).wait_send()

        @pl.when(jnp.logical_or(me == 2, me == 4))
        def _():
            for n in range(NC):
                forward(n).wait_send()


def run_kernel(*args):
    hbm = pl.BlockSpec(memory_space=pltpu.HBM)
    vmem = pl.BlockSpec(memory_space=pltpu.VMEM)
    dma, regular = pltpu.SemaphoreType.DMA, pltpu.SemaphoreType.REGULAR
    return pl.pallas_call(
        kernel,
        out_shape=(jax.ShapeDtypeStruct((NMB, 2, 128), F32), jax.ShapeDtypeStruct((1, 128), F32),
                   jax.ShapeDtypeStruct((NMB // 2, 2, ROWS, D), BF)),
        in_specs=[hbm, hbm, vmem, vmem, vmem, vmem] + [hbm] * 7 + [vmem, vmem],
        out_specs=(vmem, vmem, hbm),
        scratch_shapes=[
            pltpu.VMEM((NG, 3, D, CH), BF),
            pltpu.VMEM((13, D, CH), BF),
            pltpu.VMEM((2, NC, ROWS, CH), BF),
            pltpu.VMEM((NC, ROWS, CH), BF),
            pltpu.VMEM((ROWS, D), BF),
            pltpu.VMEM((NC, ROWS, CH), BF),
            pltpu.VMEM((8, ROWS, 1024), BF),
            pltpu.VMEM((NC, ROWS, CH), BF),
            pltpu.VMEM((2, 3, NMB, ROWS), F32),
            pltpu.VMEM((6, 8, ROWS), F32),
            dma((NG,)), dma((13,)), dma((2,)), dma((2, NC)), dma((NC,)), dma((NC,)), regular, regular,
            dma((3, NC)), dma((NC,)), dma((NC,)), dma((7,)), dma((2,)), dma((7,)), dma((6,)), dma(()), dma((8,)),
        ],
        compiler_params=pltpu.CompilerParams(vmem_limit_bytes=67043328, has_side_effects=True),
    )(*args)


def solution(mesh):
    def stage_program(tokens, targets, emb, g_final, active, g_attn, w_q, w_k, w_v, w_o, g_mlp, w_gate, w_up, w_down):
        me = lax.axis_index("pp")
        pair = jnp.where(me == FIRST, 0, jnp.where(me == 0, 1, me))
        ids = lax.dynamic_slice_in_dim(tokens, 2 * pair, 2, axis=0)
        x = emb.at[ids.reshape(2 * ROWS)].get(mode="promise_in_bounds").reshape(2, ROWS, D)
        token_loss, mean, _ = run_kernel(x, emb, jnp.broadcast_to(g_final, (8, D)), targets, g_attn.reshape(1, D), g_mlp.reshape(1, D),
          w_q.reshape(D, D), w_k.reshape(D, D), w_v.reshape(D, D), w_o.reshape(D, D),
          w_gate.reshape(D, FFN), w_up.reshape(D, FFN), w_down.reshape(FFN, D), rope_tables(), active)
        return token_loss, mean[0, :NMB]

    stack = P("pp")
    in_specs = (P("dp"), P("dp"), P(), P()) + (stack,) * 10
    return jax.shard_map(stage_program, mesh=mesh, in_specs=in_specs, out_specs=(P("dp"), P("dp")), check_vma=False)
```
